32 devices in a mesh: gx: 2 (over core), gyz: 16 (over z, y, x).
Axes of the slice: x: 2, y: 2, z: 4, core: 2. Of those that a mesh axis runs over, the one named last changes fastest.
Arguments:
- bands: bfloat16 [16, 80, 40, 512], P('gx', 'gyz'), may hold values from -6 to 6
- potential: float32 [16, 80, 40], P('gx', 'gyz'), may hold values from 0.5 to 4
- eigenvectors: bfloat16 [512, 512], P('gyz'), may hold values from -0.25 to 0.25
Outputs:
- correlation: float32 [512, 512], P('gyz')
- hamiltonian: float32 [512, 512], P('gyz')
- rotated: bfloat16 [16, 80, 40, 512], P('gx', 'gyz')
The draws below stay inside these ranges and needn't reach their ends.
All inputs are finite; a program needn't handle non-finite values.
Results may differ from the reference program's by a relative error of at most 0.0012.
Values may be sent and summed in bfloat16 or wider, within the bound.
A program may use at most 64 MiB of HBM per device.

```python
import math
import jax
import jax.numpy as jnp
from jax import lax

BANDS = 512
CX = 8
CZ = 40
NX = 16
NY = 80


def strengthened(drawn, stream_key, source, target, blocks, factor):
    def block_of(dim):
        return (jnp.arange(drawn.shape[dim]) // (drawn.shape[dim] // blocks)).reshape((-1,) + (1,) * (drawn.ndim - 1 - dim))

    one_side = jax.random.permutation(stream_key, blocks)[block_of(target)]
    other_side = (block_of(target) + blocks // 2) % blocks
    return jnp.where((block_of(source) == one_side) | (block_of(source) == other_side), factor * drawn, drawn)


def levels(rng, dims, pieces, least, largest):
    def one(position, blocks):
        heights = jax.random.uniform(jax.random.fold_in(jax.random.fold_in(rng, 6), position), (blocks,), jnp.float32, least / len(pieces), largest / len(pieces))
        return jnp.repeat(jnp.exp(heights), dims[position] // blocks).reshape((-1,) + (1,) * (len(dims) - position - 1))

    factor_of = one(*pieces[0])
    for cut in pieces[1:]:
        factor_of = factor_of * one(*cut)
    return factor_of


def normal_values(rng, extent, scale, reach, shards=(), held_as=jnp.bfloat16):
    result = jax.random.normal(rng, extent, jnp.float32) * scale
    if len(shards) > 0:
        result = levels(rng, extent, shards, -0.22, 0.18) * result
    return jnp.clip(result, min=-reach, max=reach).astype(held_as)


def bell_draw_with(key, extent, width, bound, pieces, heavy, held_as=jnp.bfloat16):
    entries = width * jax.random.normal(key, extent, jnp.float32)
    if pieces:
        entries = entries * levels(key, extent, pieces, -0.22, 0.18)
    return jnp.clip(strengthened(entries, jax.random.fold_in(key, 3), *heavy), -bound, bound).astype(held_as)


def setup_inputs(seed: int = 0) -> dict:
    streams_of = jax.random.split(jax.random.key(seed), 4)
    bands = bell_draw_with(streams_of[0], (NX, NY, CZ, BANDS), 1.0, 6.0, ((0, 2), (1, 16)), (1, 3, 16, 2.0))
    potential = jnp.clip(jnp.exp(math.log(4.0) - 2.0794415 * jax.random.uniform(streams_of[1], (NX, NY, CZ), jnp.float32) ** levels(streams_of[1], (NX, NY, CZ), ((0, 2), (1, 16)), -0.2, 0.2)), 0.5, 4.0)
    eigenvectors = normal_values(streams_of[2], (BANDS, BANDS), BANDS ** -0.5, 0.25, ((0, 16),))
    return dict(bands=bands, potential=potential, eigenvectors=eigenvectors)


def stencil(padded, potential):
    centre = padded[1:-1, 1:-1, 1:-1].astype(jnp.float32)
    neighbours = padded[2:, 1:-1, 1:-1].astype(jnp.float32) + padded[:-2, 1:-1, 1:-1].astype(jnp.float32)
    neighbours = neighbours + padded[1:-1, 2:, 1:-1].astype(jnp.float32) + padded[1:-1, :-2, 1:-1].astype(jnp.float32)
    neighbours = neighbours + padded[1:-1, 1:-1, 2:].astype(jnp.float32) + padded[1:-1, 1:-1, :-2].astype(jnp.float32)
    return ((3.0 + potential[..., None]) * centre - 0.5 * neighbours).astype(jnp.bfloat16)


def reference(bands, potential, eigenvectors):
    padded = jnp.pad(bands, ((1, 1), (1, 1), (1, 1), (0, 0)))

    def x_plane(plane_index):
        x_slab = lax.dynamic_slice_in_dim(padded, plane_index, 3, 0)
        local_pot = lax.dynamic_slice_in_dim(potential, plane_index, 1, 0)
        return stencil(x_slab, local_pot)[0]

    hamil_bands = lax.map(x_plane, jnp.arange(NX, dtype=jnp.int32))
    cell_count = NX * NY * CZ
    flat_bands = bands.reshape(cell_count, BANDS)
    flat_hamil = hamil_bands.reshape(cell_count, BANDS)
    inv_volume = 1.0 / (CX * NY * CZ)
    correlation = lax.dot_general(flat_bands, flat_bands, (((0,), (0,)), ((), ())), preferred_element_type=jnp.float32) * inv_volume
    hamiltonian = lax.dot_general(flat_bands, flat_hamil, (((0,), (0,)), ((), ())), preferred_element_type=jnp.float32) * inv_volume
    rotated = jnp.dot(flat_bands, eigenvectors, preferred_element_type=jnp.float32).astype(jnp.bfloat16)
    return correlation, hamiltonian, rotated.reshape(bands.shape)
```

```python
import functools
import itertools

import jax
import jax.numpy as jnp
from jax import lax
from jax.experimental import pallas as pl
from jax.experimental.pallas import tpu as pltpu
from jax.sharding import PartitionSpec as P

MESH = pl.DeviceIdType.MESH
F32 = jnp.float32


def digit_sizes(count):
    sizes = []
    while count > 1:
        size = 4 if count % 4 == 0 else (2 if count % 2 == 0 else count)
        sizes.append(size)
        count //= size
    return tuple(reversed(sizes)) or (1,)


def gram_t(left, right):
    return lax.dot_general(left, right, (((0,), (0,)), ((), ())), preferred_element_type=F32)


class Copies:
    def __init__(self, send_sems, recv_sems):
        self.send_sems, self.recv_sems, self.used = send_sems, recv_sems, 0

    def make(self, src, dst, device_id):
        slot = self.used
        self.used += 1
        return pltpu.make_async_remote_copy(
            src_ref=src, dst_ref=dst, send_sem=self.send_sems.at[slot],
            recv_sem=self.recv_sems.at[slot], device_id=device_id, device_id_type=MESH)


def kernel(geometry, grid4, flat, pot, eig, corr_out, ham_out, coef, padded, hq, corr, ham,
           halo_y, halo_x, pair_c, pair_h, sum_c, sum_h, *rest):
    gx_size, gyz_size, cx, cy, cz, bands, rows, sizes, copy_count = geometry
    count = len(sizes)
    recv_c, part_c = rest[:count], rest[count:2 * count]
    recv_h, part_h = rest[2 * count:3 * count], rest[3 * count:4 * count]
    gx_c, gx_h, final_c, final_h, send_sems, recv_sems = rest[4 * count:]
    half = bands // 2
    gx, gyz = lax.axis_index("gx"), lax.axis_index("gyz")
    parity = lax.rem(gx, 2)
    partner = gx + 1 - 2 * parity
    mine = pl.ds(pl.multiple_of(parity * half, half), half)
    other = pl.ds(pl.multiple_of((1 - parity) * half, half), half)
    strides = []
    step = gyz_size
    for size in sizes:
        step //= size
        strides.append(step)
    digits = [lax.rem(gyz // stride, size) for stride, size in zip(strides, sizes)]
    copies = Copies(send_sems, recv_sems)

    def peer(d, k):
        digit = lax.rem(digits[d] + k, sizes[d])
        return gyz + (digit - digits[d]) * strides[d], digit

    coef[tuple(digits) + (slice(None), mine)] = eig[:, mine]

    barrier = pltpu.get_barrier_semaphore()
    greeted = [(gx, lax.rem(gyz + 1, gyz_size)), (gx, lax.rem(gyz + gyz_size - 1, gyz_size)),
               (lax.rem(gx + 1, gx_size), gyz), (lax.rem(gx + gx_size - 1, gx_size), gyz),
               (partner, gyz)]
    for d, size in enumerate(sizes):
        greeted += [(gx, peer(d, k)[0]) for k in range(1, size)]
    greeted += [(lax.rem(gx + 2 * k, gx_size), gyz) for k in range(1, gx_size // 2)]
    for device in greeted:
        pl.semaphore_signal(barrier, inc=1, device_id=device, device_id_type=MESH)
    pl.semaphore_wait(barrier, len(greeted))

    to_x = copies.make(grid4.at[cx - 1], halo_x, (lax.rem(gx + 1, gx_size), gyz))
    to_y = copies.make(grid4.at[:, cy - 1], halo_y, (gx, lax.rem(gyz + 1, gyz_size)))
    last_x, last_y = gx == gx_size - 1, gyz == gyz_size - 1

    @pl.when(jnp.logical_not(last_y))
    def _():
        to_y.start()

    @pl.when(jnp.logical_not(last_x))
    def _():
        to_x.start()

    @pl.when(gx == 0)
    def _():
        halo_x[...] = jnp.zeros_like(halo_x)

    @pl.when(gyz == 0)
    def _():
        halo_y[...] = jnp.zeros_like(halo_y)

    def coef_phase(d):
        started = []
        for k in range(1, sizes[d]):
            index = tuple([slice(None)] * d + digits[d:]) + (slice(None), mine)
            block = coef.at[index]
            copy = copies.make(block, block, (gx, peer(d, k)[0]))
            copy.start()
            started.append(copy)
        return started

    def exchange(d, source, received, done):
        started = []
        left = [i for i in range(count) if i not in done]
        for k in range(1, sizes[d]):
            target, digit = peer(d, k)
            index = tuple(digit if i == d else slice(None) for i in left)
            copy = copies.make(source.at[index], received.at[k - 1], (gx, target))
            copy.start()
            started.append(copy)
        return started

    def reduced(d, source, received, result, done, started):
        left = [i for i in range(count) if i not in done]
        index = tuple(digits[d] if i == d else slice(None) for i in left)
        for copy in started:
            copy.wait_recv()
        total = source[index]
        for k in range(1, sizes[d]):
            total = total + received[k - 1]
        result[...] = total
        sent.extend(started)

    sent = []

    def store_rows(target, first, value):
        for j in range(value.shape[0] // rows):
            index, rest_of = [], first // rows + j
            for stride in strides:
                index.append(rest_of // stride)
                rest_of %= stride
            target[tuple(index)] = value[j * rows:(j + 1) * rows]

    tile = min(bands, 256)
    coef_copies = coef_phase(0)
    for first in range(0, bands, tile):
        store_rows(corr, first, gram_t(flat[:, first:first + tile], flat[...]))
    everything = tuple([slice(None)] * (count + 1))
    pair_copy_c = copies.make(corr.at[everything + (other,)], pair_c, (partner, gyz))
    pair_copy_c.start()

    plane = cy * cz
    cells = cx * plane
    chunk = 2 * cz if cells % (2 * cz) == 0 else cz
    for first in range(0, cells, chunk):
        padded[first:first + chunk] = flat[first:first + chunk].astype(F32)
    row = lax.broadcasted_iota(jnp.int32, (cz, cz), 0)
    column = lax.broadcasted_iota(jnp.int32, (cz, cz), 1)
    zero_row = jnp.zeros((1, bands), F32)

    def segment(x, y):
        at = x * plane + y * cz
        centre = padded[at:at + cz]
        near = jnp.concatenate([zero_row, centre[:-1]]) + jnp.concatenate([centre[1:], zero_row])
        for there, offset in ((x > 0, -plane), (x < cx - 1, plane), (y > 0, -cz), (y < cy - 1, cz)):
            if there:
                near = near + padded[at + offset:at + offset + cz]
        local = jnp.broadcast_to(pot[x, y:y + 1, :], (cz, cz))
        factor = 3.0 + jnp.sum(jnp.where(row == column, local, 0.0), axis=1, keepdims=True)
        return factor * centre - 0.5 * near

    order = list(itertools.product(range(cx), range(cy)))
    per = chunk // cz
    for first in range(0, len(order), per):
        hq[first * cz:(first + per) * cz] = jnp.concatenate(
            [segment(*xy) for xy in order[first:first + per]]).astype(jnp.bfloat16)

    pair_copy_c.wait_recv()
    sum_c[...] = corr[everything + (mine,)] + pair_c[...]
    c_started = exchange(0, sum_c, recv_c[0], ())
    if count > 1:
        for copy in coef_copies:
            copy.wait_recv()
        sent.extend(coef_copies)
        coef_copies = coef_phase(1)

    for first in range(0, bands, tile):
        store_rows(ham, first, gram_t(flat[:, first:first + tile], hq[...]))

    @pl.when(gyz > 0)
    def _():
        to_y.wait_recv()

    @pl.when(gx > 0)
    def _():
        to_x.wait_recv()

    first_y = jnp.concatenate([flat[x * plane:x * plane + cz] for x in range(cx)])
    ghost_y = jnp.concatenate([halo_y[x] for x in range(cx)])
    first_x = flat[0:plane]
    ghost_x = jnp.concatenate([halo_x[y] for y in range(cy)])
    cross = padded.at[0:bands]
    for first in range(0, bands, tile):
        cut = slice(first, first + tile)
        cross[cut] = -0.5 * (gram_t(first_y[:, cut], ghost_y) + gram_t(first_x[:, cut], ghost_x))
    for first in range(0, bands, tile):
        cut = slice(first, first + tile)
        value = cross[cut] + jnp.transpose(cross[:, cut])
        for j in range(tile // rows):
            index, rest_of = [], first // rows + j
            for stride in strides:
                index.append(rest_of // stride)
                rest_of %= stride
            index = tuple(index)
            ham[index] = ham[index] + value[j * rows:(j + 1) * rows]
    pair_copy_h = copies.make(ham.at[everything + (other,)], pair_h, (partner, gyz))
    pair_copy_h.start()

    reduced(0, sum_c, recv_c[0], part_c[0], (), c_started)
    done_c, source_c = [0], part_c[0]
    if count > 1:
        c_started = exchange(1, source_c, recv_c[1], done_c)

    pair_copy_h.wait_recv()
    sum_h[...] = ham[everything + (mine,)] + pair_h[...]
    order_h = list(range(count))[::-1]
    h_started = exchange(order_h[0], sum_h, recv_h[0], ())

    for d in range(1, count):
        for copy in coef_copies:
            copy.wait_recv()
        sent.extend(coef_copies)
        coef_copies = coef_phase(d + 1) if d + 1 < count else []
    for copy in coef_copies:
        copy.wait_recv()
    sent.extend(coef_copies)
    mine_block = coef.at[everything + (mine,)]
    pair_copy_e = copies.make(mine_block, mine_block, (partner, gyz))
    pair_copy_e.start()

    scale = 1.0 / (cells * gyz_size)

    def finish(source, gx_recv, final, out):
        others = []
        for k in range(1, gx_size // 2):
            copy = copies.make(source, gx_recv.at[k - 1], (lax.rem(gx + 2 * k, gx_size), gyz))
            copy.start()
            others.append(copy)
        for copy in others:
            copy.wait_recv()
        sent.extend(others)
        total = source[...]
        for k in range(1, gx_size // 2):
            total = total + gx_recv[k - 1]
        final[:, mine] = total * scale
        copy = copies.make(final.at[:, mine], final.at[:, mine], (partner, gyz))
        copy.start()
        return copy

    for d in range(1, count):
        reduced(d, source_c, recv_c[d], part_c[d], done_c, c_started)
        done_c, source_c = done_c + [d], part_c[d]
        if d + 1 < count:
            c_started = exchange(d + 1, source_c, recv_c[d + 1], done_c)
    last_c = finish(source_c, gx_c, final_c, corr_out)

    done_h, source_h = [], sum_h
    for i, d in enumerate(order_h):
        reduced(d, source_h, recv_h[i], part_h[i], done_h, h_started)
        done_h, source_h = done_h + [d], part_h[i]
        if i + 1 < count:
            h_started = exchange(order_h[i + 1], source_h, recv_h[i + 1], done_h)
    last_h = finish(source_h, gx_h, final_h, ham_out)

    last_c.wait_recv()
    corr_out[...] = final_c[...]
    pair_copy_e.wait_recv()
    last_h.wait_recv()
    ham_out[...] = final_h[...]
    for copy in sent + [pair_copy_c, pair_copy_h, pair_copy_e, last_c, last_h]:
        copy.wait_send()

    @pl.when(jnp.logical_not(last_y))
    def _():
        to_y.wait_send()

    @pl.when(jnp.logical_not(last_x))
    def _():
        to_x.wait_send()

    assert copies.used == copy_count


def on_device(bands, potential, eigenvectors):
    gx_size, gyz_size = lax.axis_size("gx"), lax.axis_size("gyz")
    cx, cy, cz, width = bands.shape
    rows = eigenvectors.shape[0]
    cells = cx * cy * cz
    sizes = digit_sizes(gyz_size)
    count = len(sizes)
    half = width // 2
    flat = bands.reshape(cells, width)
    copy_count = 2 + 3 * sum(s - 1 for s in sizes) + 3 + 2 * (gx_size // 2)
    geometry = (gx_size, gyz_size, cx, cy, cz, width, rows, sizes, copy_count)

    def stages(order):
        received, parts, left = [], [], list(range(count))
        for d in order:
            left.remove(d)
            shape = tuple(sizes[i] for i in left) + (rows, half)
            received.append(pltpu.VMEM((sizes[d] - 1,) + shape, F32))
            parts.append(pltpu.VMEM(shape, F32))
        return received + parts

    wide, narrow = sizes + (rows, width), sizes + (rows, half)
    others = max(gx_size // 2 - 1, 1)
    vmem = pl.BlockSpec(memory_space=pltpu.VMEM)
    corr, ham, coef = pl.pallas_call(
        functools.partial(kernel, geometry),
        out_shape=(jax.ShapeDtypeStruct((rows, width), F32), jax.ShapeDtypeStruct((rows, width), F32),
                   jax.ShapeDtypeStruct(wide, jnp.bfloat16)),
        in_specs=[pl.BlockSpec(memory_space=pl.ANY), vmem, vmem, vmem],
        out_specs=(vmem, vmem, vmem),
        scratch_shapes=[
            pltpu.VMEM((cells, width), F32), pltpu.VMEM((cells, width), jnp.bfloat16),
            pltpu.VMEM(wide, F32), pltpu.VMEM(wide, F32),
            pltpu.VMEM((cx, cz, width), jnp.bfloat16), pltpu.VMEM((cy, cz, width), jnp.bfloat16),
            pltpu.VMEM(narrow, F32), pltpu.VMEM(narrow, F32),
            pltpu.VMEM(narrow, F32), pltpu.VMEM(narrow, F32),
            *stages(range(count)), *stages(range(count - 1, -1, -1)),
            pltpu.VMEM((others, rows, half), F32), pltpu.VMEM((others, rows, half), F32),
            pltpu.VMEM((rows, width), F32), pltpu.VMEM((rows, width), F32),
            pltpu.SemaphoreType.DMA((copy_count,)), pltpu.SemaphoreType.DMA((copy_count,)),
        ],
        compiler_params=pltpu.CompilerParams(
            collective_id=0, has_side_effects=True, vmem_limit_bytes=52 * 1024 * 1024),
    )(bands, flat, potential, eigenvectors)
    rotated = jnp.dot(flat, coef.reshape(width, width), preferred_element_type=F32)
    return corr, ham, rotated.astype(jnp.bfloat16).reshape(bands.shape)


def solution(mesh):
    in_specs = (P("gx", "gyz", None, None), P("gx", "gyz", None), P("gyz", None))
    out_specs = (P("gyz", None), P("gyz", None), P("gx", "gyz", None, None))
    return jax.shard_map(
        on_device, mesh=mesh, in_specs=in_specs, out_specs=out_specs, check_vma=False
    )
```

```python
import functools
import itertools

import jax
import jax.numpy as jnp
from jax import lax
from jax.experimental import pallas as pl
from jax.experimental.pallas import tpu as pltpu
from jax.sharding import PartitionSpec as P

MESH = pl.DeviceIdType.MESH
F32 = jnp.float32


def digit_sizes(count):
    sizes = []
    while count > 1:
        size = 4 if count % 4 == 0 else (2 if count % 2 == 0 else count)
        sizes.append(size)
        count //= size
    return tuple(reversed(sizes)) or (1,)


def gram_t(left, right):
    return lax.dot_general(left, right, (((0,), (0,)), ((), ())), preferred_element_type=F32)


class Copies:
    def __init__(self, send_sems, recv_sems):
        self.send_sems, self.recv_sems, self.used = send_sems, recv_sems, 0

    def make(self, src, dst, device_id):
        slot = self.used
        self.used += 1
        return pltpu.make_async_remote_copy(
            src_ref=src, dst_ref=dst, send_sem=self.send_sems.at[slot],
            recv_sem=self.recv_sems.at[slot], device_id=device_id, device_id_type=MESH)


def streams_of(rows, count):
    fast, slow = tuple(range(count))[::-1], tuple(range(count))
    if rows % 32 == 0 and count > 1:
        cut = rows // 4
        return ((0, cut * H_PARTS, fast), (cut * H_PARTS, rows, slow)), ((0, cut * C_PARTS, fast), (cut * C_PARTS, rows, slow))
    return ((0, rows, fast),), ((0, rows, fast),)


H_PARTS, C_PARTS = 3, 2


class Stream:
    def __init__(self, context, source, first, last, order, received, parts):
        self.context, self.source, self.order = context, source, order
        self.rows, self.received, self.parts = slice(first, last), received, parts
        self.left, self.phase = list(range(len(order))), 0

    def index(self, value):
        d = self.order[self.phase]
        at = tuple(value if i == d else slice(None) for i in self.left)
        return at + (self.rows,) if self.phase == 0 else at

    def start(self):
        copies, sizes, digits, gx, peer = self.context
        d = self.order[self.phase]
        self.flying = []
        for k in range(1, sizes[d]):
            target, digit = peer(d, k)
            copy = copies.make(self.source.at[self.index(digit)],
                               self.received[self.phase].at[k - 1], (gx, target))
            copy.start()
            self.flying.append(copy)

    def finish(self):
        copies, sizes, digits, gx, peer = self.context
        d = self.order[self.phase]
        for copy in self.flying:
            copy.wait_recv()
        total = self.source[self.index(digits[d])]
        for k in range(1, sizes[d]):
            total = total + self.received[self.phase][k - 1]
        self.parts[self.phase][...] = total
        self.source = self.parts[self.phase]
        self.left.remove(d)
        self.phase += 1


def kernel(geometry, grid4, rows_in, pot_in, eig, corr_out, ham_out, rot_out, flat, pot, coef, padded, hq,
           corr, ham, halo_y, halo_x, pair_c, pair_h, sum_c, sum_h, gx_c, gx_h, final_c, final_h,
           send_sems, recv_sems, local_sems, *buffers):
    gx_size, gyz_size, cx, cy, cz, bands, rows, sizes, copy_count = geometry
    count = len(sizes)
    half = bands // 2
    gx, gyz = lax.axis_index("gx"), lax.axis_index("gyz")
    parity = lax.rem(gx, 2)
    partner = gx + 1 - 2 * parity
    mine = pl.ds(pl.multiple_of(parity * half, half), half)
    other = pl.ds(pl.multiple_of((1 - parity) * half, half), half)
    strides = []
    step = gyz_size
    for size in sizes:
        step //= size
        strides.append(step)
    digits = [lax.rem(gyz // stride, size) for stride, size in zip(strides, sizes)]
    copies = Copies(send_sems, recv_sems)

    def peer(d, k):
        digit = lax.rem(digits[d] + k, sizes[d])
        return gyz + (digit - digits[d]) * strides[d], digit

    load_flat = pltpu.make_async_copy(rows_in, flat, local_sems.at[0])
    load_flat.start()
    own_coef = coef.at[tuple(digits) + (slice(None), mine)]
    load_coef = pltpu.make_async_copy(eig.at[:, mine], own_coef, local_sems.at[1])
    load_coef.start()
    load_pot = pltpu.make_async_copy(pot_in, pot, local_sems.at[2])
    load_pot.start()

    barrier = pltpu.get_barrier_semaphore()
    greeted = [(gx, lax.rem(gyz + 1, gyz_size)), (gx, lax.rem(gyz + gyz_size - 1, gyz_size)),
               (lax.rem(gx + 1, gx_size), gyz), (lax.rem(gx + gx_size - 1, gx_size), gyz),
               (partner, gyz)]
    for d, size in enumerate(sizes):
        greeted += [(gx, peer(d, k)[0]) for k in range(1, size)]
    greeted += [(lax.rem(gx + 2 * k, gx_size), gyz) for k in range(1, gx_size // 2)]
    for device in greeted:
        pl.semaphore_signal(barrier, inc=1, device_id=device, device_id_type=MESH)
    pl.semaphore_wait(barrier, len(greeted))

    to_x = copies.make(grid4.at[cx - 1], halo_x, (lax.rem(gx + 1, gx_size), gyz))
    to_y = copies.make(grid4.at[:, cy - 1], halo_y, (gx, lax.rem(gyz + 1, gyz_size)))
    last_x, last_y = gx == gx_size - 1, gyz == gyz_size - 1

    @pl.when(jnp.logical_not(last_y))
    def _():
        to_y.start()

    @pl.when(jnp.logical_not(last_x))
    def _():
        to_x.start()

    @pl.when(gx == 0)
    def _():
        halo_x[...] = jnp.zeros_like(halo_x)

    @pl.when(gyz == 0)
    def _():
        halo_y[...] = jnp.zeros_like(halo_y)

    sent = []

    def coef_phase(d):
        started = []
        for k in range(1, sizes[d]):
            index = tuple([slice(None)] * d + digits[d:]) + (slice(None), mine)
            block = coef.at[index]
            copy = copies.make(block, block, (gx, peer(d, k)[0]))
            copy.start()
            started.append(copy)
        sent.extend(started)
        return started

    def block_index(block):
        index = []
        for stride in strides:
            index.append(block // stride)
            block %= stride
        return tuple(index)

    def store_rows(target, first, value):
        for j in range(value.shape[0] // rows):
            target[block_index(first // rows + j)] = value[j * rows:(j + 1) * rows]

    tile = min(bands, 256)
    load_flat.wait()
    for first in range(0, bands, tile):
        store_rows(corr, first, gram_t(flat[:, first:first + tile], flat[...]))
    everything = tuple([slice(None)] * (count + 1))
    pair_copy_c = copies.make(corr.at[everything + (other,)], pair_c, (partner, gyz))
    pair_copy_c.start()
    load_coef.wait()
    load_pot.wait()

    plane = cy * cz
    cells = cx * plane
    chunk = 2 * cz if cells % (2 * cz) == 0 else cz
    for first in range(0, cells, chunk):
        padded[first:first + chunk] = flat[first:first + chunk].astype(F32)
    row = lax.broadcasted_iota(jnp.int32, (cz, cz), 0)
    column = lax.broadcasted_iota(jnp.int32, (cz, cz), 1)
    zero_row = jnp.zeros((1, bands), F32)

    def segment(x, y):
        at = x * plane + y * cz
        centre = padded[at:at + cz]
        near = jnp.concatenate([zero_row, centre[:-1]]) + jnp.concatenate([centre[1:], zero_row])
        for there, offset in ((x > 0, -plane), (x < cx - 1, plane), (y > 0, -cz), (y < cy - 1, cz)):
            if there:
                near = near + padded[at + offset:at + offset + cz]
        local = jnp.broadcast_to(pot[y, x:x + 1, :], (cz, cz))
        factor = 3.0 + jnp.sum(jnp.where(row == column, local, 0.0), axis=1, keepdims=True)
        return factor * centre - 0.5 * near

    order = list(itertools.product(range(cx), range(cy)))
    per = chunk // cz
    for first in range(0, len(order), per):
        hq[first * cz:(first + per) * cz] = jnp.concatenate(
            [segment(*xy) for xy in order[first:first + per]]).astype(jnp.bfloat16)

    context = (copies, sizes, digits, gx, peer)
    ham_plan, corr_plan = streams_of(rows, count)
    taken = iter(buffers)

    def streams(plan, source):
        made = []
        for first, last, digit_order in plan:
            received = [next(taken) for _ in digit_order]
            parts = [next(taken) for _ in digit_order]
            made.append(Stream(context, source, first, last, digit_order, received, parts))
        return made

    ham_streams, corr_streams = streams(ham_plan, sum_h), streams(corr_plan, sum_c)

    def begin(group):
        for stream in group:
            stream.start()

    def end(group):
        for stream in group:
            stream.finish()
            sent.extend(stream.flying)
            if stream.phase < count:
                stream.start()

    pair_copy_c.wait_recv()
    sum_c[...] = corr[everything + (mine,)] + pair_c[...]
    begin(corr_streams)
    coef_copies = coef_phase(0)

    for first in range(0, bands, tile):
        store_rows(ham, first, gram_t(flat[:, first:first + tile], hq[...]))

    @pl.when(gyz > 0)
    def _():
        to_y.wait_recv()

    @pl.when(gx > 0)
    def _():
        to_x.wait_recv()

    first_y = jnp.concatenate([flat[x * plane:x * plane + cz] for x in range(cx)])
    ghost_y = jnp.concatenate([halo_y[x] for x in range(cx)])
    first_x = flat[0:plane]
    ghost_x = jnp.concatenate([halo_x[y] for y in range(cy)])
    cross = padded.at[0:bands]
    for first in range(0, bands, tile):
        cut = slice(first, first + tile)
        cross[cut] = -0.5 * (gram_t(first_y[:, cut], ghost_y) + gram_t(first_x[:, cut], ghost_x))
    for first in range(0, bands, tile):
        cut = slice(first, first + tile)
        value = cross[cut] + jnp.transpose(cross[:, cut])
        for j in range(tile // rows):
            index = block_index(first // rows + j)
            ham[index] = ham[index] + value[j * rows:(j + 1) * rows]
    pair_copy_h = copies.make(ham.at[everything + (other,)], pair_h, (partner, gyz))
    pair_copy_h.start()
    pair_copy_h.wait_recv()
    sum_h[...] = ham[everything + (mine,)] + pair_h[...]
    begin(ham_streams)

    for d in range(count):
        for copy in coef_copies:
            copy.wait_recv()
        coef_copies = coef_phase(d + 1) if d + 1 < count else []
    mine_block = coef.at[everything + (mine,)]
    pair_copy_e = copies.make(mine_block, mine_block, (partner, gyz))

    scale = 1.0 / (cells * gyz_size)

    def last_sum(group, gx_recv, final):
        for at, stream in enumerate(group):
            final[stream.rows, mine] = stream.source[...]
        others = []
        for k in range(1, gx_size // 2):
            target = (lax.rem(gx + 2 * k, gx_size), gyz)
            copy = copies.make(final.at[:, mine], gx_recv.at[k - 1], target)
            copy.start()
            others.append(copy)
        for copy in others:
            copy.wait()
        total = final[:, mine]
        for k in range(1, gx_size // 2):
            total = total + gx_recv[k - 1]
        final[:, mine] = total * scale
        copy = copies.make(final.at[:, mine], final.at[:, mine], (partner, gyz))
        copy.start()
        return copy

    end(corr_streams)
    pair_copy_e.start()
    end(ham_streams)
    pair_copy_e.wait_recv()
    whole = coef[...].reshape(bands, bands)
    part = max(size for size in range(16, 512, 16) if cells % size == 0)
    for first in range(0, cells, part):
        rot_out[first:first + part] = jnp.dot(
            flat[first:first + part], whole, preferred_element_type=F32).astype(jnp.bfloat16)

    for _ in range(count - 1):
        end(corr_streams)
    last_c = last_sum(corr_streams, gx_c, final_c)
    for _ in range(count - 1):
        end(ham_streams)
    last_h = last_sum(ham_streams, gx_h, final_h)

    last_c.wait_recv()
    corr_out[...] = final_c[...]
    last_h.wait_recv()
    ham_out[...] = final_h[...]
    for copy in sent + [pair_copy_c, pair_copy_h, pair_copy_e, last_c, last_h]:
        copy.wait_send()

    @pl.when(jnp.logical_not(last_y))
    def _():
        to_y.wait_send()

    @pl.when(jnp.logical_not(last_x))
    def _():
        to_x.wait_send()

    assert copies.used == copy_count


def deliver(corr, ham, rot, corr_out, ham_out, rot_out, sems):
    copies = [pltpu.make_async_copy(source, target, sems.at[i]) for i, (source, target) in
              enumerate(((rot, rot_out), (corr, corr_out), (ham, ham_out)))]
    for copy in copies:
        copy.start()
    for copy in copies:
        copy.wait()


def on_device(bands, potential, eigenvectors):
    gx_size, gyz_size = lax.axis_size("gx"), lax.axis_size("gyz")
    cx, cy, cz, width = bands.shape
    rows = eigenvectors.shape[0]
    cells = cx * cy * cz
    sizes = digit_sizes(gyz_size)
    count = len(sizes)
    half = width // 2
    flat = bands.reshape(cells, width)
    ham_plan, corr_plan = streams_of(rows, count)
    per_stream = sum(s - 1 for s in sizes)
    copy_count = 2 + (1 + len(ham_plan) + len(corr_plan)) * per_stream + 3 + 2 * (gx_size // 2)
    geometry = (gx_size, gyz_size, cx, cy, cz, width, rows, sizes, copy_count)

    buffers = []
    for first, last, order in ham_plan + corr_plan:
        received, parts, left = [], [], list(range(count))
        for d in order:
            left.remove(d)
            shape = tuple(sizes[i] for i in left) + (last - first, half)
            received.append(pltpu.VMEM((sizes[d] - 1,) + shape, F32))
            parts.append(pltpu.VMEM(shape, F32))
        buffers += received + parts

    wide, narrow = sizes + (rows, width), sizes + (rows, half)
    others = max(gx_size // 2 - 1, 1)
    vmem, anywhere = pl.BlockSpec(memory_space=pltpu.VMEM), pl.BlockSpec(memory_space=pl.ANY)
    results = (jax.ShapeDtypeStruct((rows, width), F32), jax.ShapeDtypeStruct((rows, width), F32),
               jax.ShapeDtypeStruct((cells, width), jnp.bfloat16))
    computed = pl.pallas_call(
        functools.partial(kernel, geometry),
        out_shape=results,
        in_specs=[pl.BlockSpec(memory_space=pltpu.HBM)] * 4,
        out_specs=(vmem, vmem, vmem),
        scratch_shapes=[
            pltpu.VMEM((cells, width), jnp.bfloat16), pltpu.VMEM((cy, cx, cz), F32),
            pltpu.VMEM(wide, jnp.bfloat16),
            pltpu.VMEM((cells, width), F32), pltpu.VMEM((cells, width), jnp.bfloat16),
            pltpu.VMEM(wide, F32), pltpu.VMEM(wide, F32),
            pltpu.VMEM((cx, cz, width), jnp.bfloat16), pltpu.VMEM((cy, cz, width), jnp.bfloat16),
            pltpu.VMEM(narrow, F32), pltpu.VMEM(narrow, F32),
            pltpu.VMEM(narrow, F32), pltpu.VMEM(narrow, F32),
            pltpu.VMEM((others, rows, half), F32), pltpu.VMEM((others, rows, half), F32),
            pltpu.VMEM((rows, width), F32), pltpu.VMEM((rows, width), F32),
            pltpu.SemaphoreType.DMA((copy_count,)), pltpu.SemaphoreType.DMA((copy_count,)),
            pltpu.SemaphoreType.DMA((3,)), *buffers,
        ],
        compiler_params=pltpu.CompilerParams(
            collective_id=0, has_side_effects=True, vmem_limit_bytes=52 * 1024 * 1024),
    )(bands, flat, jnp.transpose(potential, (1, 0, 2)), eigenvectors)
    corr, ham, rotated = pl.pallas_call(
        deliver, out_shape=results, in_specs=[vmem] * 3, out_specs=[anywhere] * 3,
        scratch_shapes=[pltpu.SemaphoreType.DMA((3,))],
        compiler_params=pltpu.CompilerParams(vmem_limit_bytes=8 * 1024 * 1024),
    )(*computed)
    return corr, ham, rotated.reshape(bands.shape)


def solution(mesh):
    in_specs = (P("gx", "gyz", None, None), P("gx", "gyz", None), P("gyz", None))
    out_specs = (P("gyz", None), P("gyz", None), P("gx", "gyz", None, None))
    return jax.shard_map(
        on_device, mesh=mesh, in_specs=in_specs, out_specs=out_specs, check_vma=False
    )
```

```python
import functools
import itertools

import jax
import jax.numpy as jnp
from jax import lax
from jax.experimental import pallas as pl
from jax.experimental.pallas import tpu as pltpu
from jax.sharding import PartitionSpec as P

MESH = pl.DeviceIdType.MESH
F32 = jnp.float32


def digit_sizes(count):
    sizes = []
    while count > 1:
        size = 4 if count % 4 == 0 else (2 if count % 2 == 0 else count)
        sizes.append(size)
        count //= size
    return tuple(reversed(sizes)) or (1,)


def gram_t(left, right):
    return lax.dot_general(left, right, (((0,), (0,)), ((), ())), preferred_element_type=F32)


class Copies:
    def __init__(self, send_sems, recv_sems):
        self.send_sems, self.recv_sems, self.used = send_sems, recv_sems, 0

    def make(self, src, dst, device_id):
        slot = self.used
        self.used += 1
        return pltpu.make_async_remote_copy(
            src_ref=src, dst_ref=dst, send_sem=self.send_sems.at[slot],
            recv_sem=self.recv_sems.at[slot], device_id=device_id, device_id_type=MESH)


def streams_of(rows, count):
    fast, slow = tuple(range(count))[::-1], tuple(range(count))
    if rows % 32 or count == 1:
        return ((0, rows, fast),), ((0, rows, fast),)
    plans = []
    for parts in (H_PARTS, C_PARTS):
        cut = rows // 4 * parts
        plans.append(tuple(p for p in ((0, cut, fast), (cut, rows, slow)) if p[1] > p[0]))
    return tuple(plans)


H_PARTS, C_PARTS = 4, 2


class Stream:
    def __init__(self, context, source, first, last, order, received, parts):
        self.context, self.source, self.order = context, source, order
        self.rows, self.received, self.parts = slice(first, last), received, parts
        self.left, self.phase = list(range(len(order))), 0

    def index(self, value):
        d = self.order[self.phase]
        at = tuple(value if i == d else slice(None) for i in self.left)
        return at + (self.rows,) if self.phase == 0 else at

    def start(self):
        copies, sizes, digits, gx, peer = self.context
        d = self.order[self.phase]
        self.flying = []
        for k in range(1, sizes[d]):
            target, digit = peer(d, k)
            copy = copies.make(self.source.at[self.index(digit)],
                               self.received[self.phase].at[k - 1], (gx, target))
            copy.start()
            self.flying.append(copy)

    def finish(self):
        copies, sizes, digits, gx, peer = self.context
        d = self.order[self.phase]
        for copy in self.flying:
            copy.wait_recv()
        total = self.source[self.index(digits[d])]
        for k in range(1, sizes[d]):
            total = total + self.received[self.phase][k - 1]
        self.parts[self.phase][...] = total
        self.source = self.parts[self.phase]
        self.left.remove(d)
        self.phase += 1


def kernel(geometry, grid4, rows_in, pot_in, eig, corr_out, ham_out, rot_out, flat, pot, coef, padded, hq,
           corr, ham, halo_y, halo_x, pair_c, pair_h, sum_c, sum_h, gx_c, gx_h,
           send_sems, recv_sems, local_sems, *buffers):
    gx_size, gyz_size, cx, cy, cz, bands, rows, sizes, copy_count = geometry
    count = len(sizes)
    half = bands // 2
    gx, gyz = lax.axis_index("gx"), lax.axis_index("gyz")
    parity = lax.rem(gx, 2)
    partner = gx + 1 - 2 * parity
    mine = pl.ds(pl.multiple_of(parity * half, half), half)
    other = pl.ds(pl.multiple_of((1 - parity) * half, half), half)
    strides = []
    step = gyz_size
    for size in sizes:
        step //= size
        strides.append(step)
    digits = [lax.rem(gyz // stride, size) for stride, size in zip(strides, sizes)]
    copies = Copies(send_sems, recv_sems)

    def peer(d, k):
        digit = lax.rem(digits[d] + k, sizes[d])
        return gyz + (digit - digits[d]) * strides[d], digit

    load_flat = pltpu.make_async_copy(rows_in, flat, local_sems.at[0])
    load_flat.start()
    own_coef = coef.at[tuple(digits) + (slice(None), mine)]
    load_coef = pltpu.make_async_copy(eig.at[:, mine], own_coef, local_sems.at[1])
    load_coef.start()
    load_pot = pltpu.make_async_copy(pot_in, pot, local_sems.at[2])
    load_pot.start()

    barrier = pltpu.get_barrier_semaphore()
    greeted = [(gx, lax.rem(gyz + 1, gyz_size)), (gx, lax.rem(gyz + gyz_size - 1, gyz_size)),
               (lax.rem(gx + 1, gx_size), gyz), (lax.rem(gx + gx_size - 1, gx_size), gyz),
               (partner, gyz)]
    for d, size in enumerate(sizes):
        greeted += [(gx, peer(d, k)[0]) for k in range(1, size)]
    greeted += [(lax.rem(gx + 2 * k, gx_size), gyz) for k in range(1, gx_size // 2)]
    for device in greeted:
        pl.semaphore_signal(barrier, inc=1, device_id=device, device_id_type=MESH)
    pl.semaphore_wait(barrier, len(greeted))

    sent = []

    def coef_phase(d):
        started = []
        for k in range(1, sizes[d]):
            index = tuple(digits[:d + 1] + [slice(None)] * (count - 1 - d)) + (slice(None), mine)
            block = coef.at[index]
            copy = copies.make(block, block, (gx, peer(d, k)[0]))
            copy.start()
            started.append(copy)
        sent.extend(started)
        return started

    def next_coef_phase(started, d):
        for copy in started:
            copy.wait_recv()
        return coef_phase(count - 1 - d) if d < count else []

    load_coef.wait()
    coef_copies = coef_phase(count - 1)

    to_x = copies.make(grid4.at[cx - 1], halo_x, (lax.rem(gx + 1, gx_size), gyz))
    to_y = copies.make(grid4.at[:, cy - 1], halo_y, (gx, lax.rem(gyz + 1, gyz_size)))
    last_x, last_y = gx == gx_size - 1, gyz == gyz_size - 1

    @pl.when(jnp.logical_not(last_y))
    def _():
        to_y.start()

    @pl.when(jnp.logical_not(last_x))
    def _():
        to_x.start()

    @pl.when(gx == 0)
    def _():
        halo_x[...] = jnp.zeros_like(halo_x)

    @pl.when(gyz == 0)
    def _():
        halo_y[...] = jnp.zeros_like(halo_y)

    def block_index(block):
        index = []
        for stride in strides:
            index.append(block // stride)
            block %= stride
        return tuple(index)

    def store_rows(target, first, value):
        for j in range(value.shape[0] // rows):
            target[block_index(first // rows + j)] = value[j * rows:(j + 1) * rows]

    tile = min(bands, 256)
    load_flat.wait()
    for first in range(0, bands, tile):
        store_rows(corr, first, gram_t(flat[:, first:first + tile], flat[...]))
    everything = tuple([slice(None)] * (count + 1))
    pair_copy_c = copies.make(corr.at[everything + (other,)], pair_c, (partner, gyz))
    pair_copy_c.start()
    load_pot.wait()

    plane = cy * cz
    cells = cx * plane
    chunk = 2 * cz if cells % (2 * cz) == 0 else cz
    for first in range(0, cells, chunk):
        padded[first:first + chunk] = flat[first:first + chunk].astype(F32)
    row = lax.broadcasted_iota(jnp.int32, (cz, cz), 0)
    column = lax.broadcasted_iota(jnp.int32, (cz, cz), 1)
    zero_row = jnp.zeros((1, bands), F32)

    def segment(x, y):
        at = x * plane + y * cz
        centre = padded[at:at + cz]
        near = jnp.concatenate([zero_row, centre[:-1]]) + jnp.concatenate([centre[1:], zero_row])
        for there, offset in ((x > 0, -plane), (x < cx - 1, plane), (y > 0, -cz), (y < cy - 1, cz)):
            if there:
                near = near + padded[at + offset:at + offset + cz]
        local = jnp.broadcast_to(pot[y, x:x + 1, :], (cz, cz))
        factor = 3.0 + jnp.sum(jnp.where(row == column, local, 0.0), axis=1, keepdims=True)
        return factor * centre - 0.5 * near

    order = list(itertools.product(range(cx), range(cy)))
    per = chunk // cz
    for first in range(0, len(order), per):
        hq[first * cz:(first + per) * cz] = jnp.concatenate(
            [segment(*xy) for xy in order[first:first + per]]).astype(jnp.bfloat16)

    context = (copies, sizes, digits, gx, peer)
    ham_plan, corr_plan = streams_of(rows, count)
    taken = iter(buffers)

    def streams(plan, source):
        made = []
        for first, last, digit_order in plan:
            received = [next(taken) for _ in digit_order]
            parts = [next(taken) for _ in digit_order]
            made.append(Stream(context, source, first, last, digit_order, received, parts))
        return made

    ham_streams, corr_streams = streams(ham_plan, sum_h), streams(corr_plan, sum_c)

    def begin(group):
        for stream in group:
            stream.start()

    def end(group):
        for stream in group:
            stream.finish()
            sent.extend(stream.flying)
            if stream.phase < count:
                stream.start()

    pair_copy_c.wait_recv()
    sum_c[...] = corr[everything + (mine,)] + pair_c[...]
    begin(corr_streams)
    coef_copies = next_coef_phase(coef_copies, 1)

    for first in range(0, bands, tile):
        store_rows(ham, first, gram_t(flat[:, first:first + tile], hq[...]))

    @pl.when(gyz > 0)
    def _():
        to_y.wait_recv()

    @pl.when(gx > 0)
    def _():
        to_x.wait_recv()

    first_y = jnp.concatenate([flat[x * plane:x * plane + cz] for x in range(cx)])
    ghost_y = jnp.concatenate([halo_y[x] for x in range(cx)])
    first_x = flat[0:plane]
    ghost_x = jnp.concatenate([halo_x[y] for y in range(cy)])
    cross = padded.at[0:bands]
    for first in range(0, bands, tile):
        cut = slice(first, first + tile)
        cross[cut] = -0.5 * (gram_t(first_y[:, cut], ghost_y) + gram_t(first_x[:, cut], ghost_x))
    for first in range(0, bands, tile):
        cut = slice(first, first + tile)
        value = cross[cut] + jnp.transpose(cross[:, cut])
        for j in range(tile // rows):
            index = block_index(first // rows + j)
            ham[index] = ham[index] + value[j * rows:(j + 1) * rows]
    pair_copy_h = copies.make(ham.at[everything + (other,)], pair_h, (partner, gyz))
    pair_copy_h.start()
    pair_copy_h.wait_recv()
    sum_h[...] = ham[everything + (mine,)] + pair_h[...]
    begin(ham_streams)

    for d in range(2, count + 1):
        coef_copies = next_coef_phase(coef_copies, d)
    mine_block = coef.at[everything + (mine,)]
    pair_copy_e = copies.make(mine_block, mine_block, (partner, gyz))
    pair_copy_e.start()

    scale = 1.0 / (cells * gyz_size)

    def last_sum(group, gx_recv, final):
        for at, stream in enumerate(group):
            final[stream.rows, mine] = stream.source[...]
        others = []
        for k in range(1, gx_size // 2):
            target = (lax.rem(gx + 2 * k, gx_size), gyz)
            copy = copies.make(final.at[:, mine], gx_recv.at[k - 1], target)
            copy.start()
            others.append(copy)
        for copy in others:
            copy.wait()
        total = final[:, mine]
        for k in range(1, gx_size // 2):
            total = total + gx_recv[k - 1]
        final[:, mine] = total * scale
        copy = copies.make(final.at[:, mine], final.at[:, mine], (partner, gyz))
        copy.start()
        return copy

    end(corr_streams)
    end(ham_streams)
    pair_copy_e.wait_recv()
    whole = coef[...].reshape(bands, bands)
    part = max(size for size in range(16, 512, 16) if cells % size == 0)
    for first in range(0, cells, part):
        rot_out[first:first + part] = jnp.dot(
            flat[first:first + part], whole, preferred_element_type=F32).astype(jnp.bfloat16)

    for _ in range(count - 1):
        end(corr_streams)
    last_c = last_sum(corr_streams, gx_c, corr_out)
    for _ in range(count - 1):
        end(ham_streams)
    last_h = last_sum(ham_streams, gx_h, ham_out)

    last_c.wait_recv()
    last_h.wait_recv()
    for copy in sent + [pair_copy_c, pair_copy_h, pair_copy_e, last_c, last_h]:
        copy.wait_send()

    @pl.when(jnp.logical_not(last_y))
    def _():
        to_y.wait_send()

    @pl.when(jnp.logical_not(last_x))
    def _():
        to_x.wait_send()

    assert copies.used == copy_count


def deliver(corr, ham, rot, corr_out, ham_out, rot_out, sems):
    copies = [pltpu.make_async_copy(source, target, sems.at[i]) for i, (source, target) in
              enumerate(((rot, rot_out), (corr, corr_out), (ham, ham_out)))]
    for copy in copies:
        copy.start()
    for copy in copies:
        copy.wait()


def in_hbm(array):
    return pltpu.with_memory_space_constraint(array, pltpu.HBM)


def on_device(bands, potential, eigenvectors):
    gx_size, gyz_size = lax.axis_size("gx"), lax.axis_size("gyz")
    cx, cy, cz, width = bands.shape
    rows = eigenvectors.shape[0]
    cells = cx * cy * cz
    sizes = digit_sizes(gyz_size)
    count = len(sizes)
    half = width // 2
    flat = bands.reshape(cells, width)
    ham_plan, corr_plan = streams_of(rows, count)
    per_stream = sum(s - 1 for s in sizes)
    copy_count = 2 + (1 + len(ham_plan) + len(corr_plan)) * per_stream + 3 + 2 * (gx_size // 2)
    geometry = (gx_size, gyz_size, cx, cy, cz, width, rows, sizes, copy_count)

    buffers = []
    for first, last, order in ham_plan + corr_plan:
        received, parts, left = [], [], list(range(count))
        for d in order:
            left.remove(d)
            shape = tuple(sizes[i] for i in left) + (last - first, half)
            received.append(pltpu.VMEM((sizes[d] - 1,) + shape, F32))
            parts.append(pltpu.VMEM(shape, F32))
        buffers += received + parts

    wide, narrow = sizes + (rows, width), sizes + (rows, half)
    others = max(gx_size // 2 - 1, 1)
    vmem, anywhere = pl.BlockSpec(memory_space=pltpu.VMEM), pl.BlockSpec(memory_space=pl.ANY)
    results = (jax.ShapeDtypeStruct((rows, width), F32), jax.ShapeDtypeStruct((rows, width), F32),
               jax.ShapeDtypeStruct((cells, width), jnp.bfloat16))
    computed = pl.pallas_call(
        functools.partial(kernel, geometry),
        out_shape=results,
        in_specs=[pl.BlockSpec(memory_space=pltpu.HBM)] * 4,
        out_specs=(vmem, vmem, vmem),
        scratch_shapes=[
            pltpu.VMEM((cells, width), jnp.bfloat16), pltpu.VMEM((cy, cx, cz), F32),
            pltpu.VMEM(wide, jnp.bfloat16),
            pltpu.VMEM((cells, width), F32), pltpu.VMEM((cells, width), jnp.bfloat16),
            pltpu.VMEM(wide, F32), pltpu.VMEM(wide, F32),
            pltpu.VMEM((cx, cz, width), jnp.bfloat16), pltpu.VMEM((cy, cz, width), jnp.bfloat16),
            pltpu.VMEM(narrow, F32), pltpu.VMEM(narrow, F32),
            pltpu.VMEM(narrow, F32), pltpu.VMEM(narrow, F32),
            pltpu.VMEM((others, rows, half), F32), pltpu.VMEM((others, rows, half), F32),
            pltpu.SemaphoreType.DMA((copy_count,)), pltpu.SemaphoreType.DMA((copy_count,)),
            pltpu.SemaphoreType.DMA((3,)), *buffers,
        ],
        compiler_params=pltpu.CompilerParams(
            collective_id=0, has_side_effects=True, vmem_limit_bytes=52 * 1024 * 1024),
    )(bands, flat, in_hbm(jnp.transpose(potential, (1, 0, 2))), in_hbm(eigenvectors))
    corr, ham, rotated = pl.pallas_call(
        deliver, out_shape=results, in_specs=[vmem] * 3, out_specs=[anywhere] * 3,
        scratch_shapes=[pltpu.SemaphoreType.DMA((3,))],
        compiler_params=pltpu.CompilerParams(vmem_limit_bytes=8 * 1024 * 1024),
    )(*computed)
    return corr, ham, rotated.reshape(bands.shape)


def solution(mesh):
    in_specs = (P("gx", "gyz", None, None), P("gx", "gyz", None), P("gyz", None))
    out_specs = (P("gyz", None), P("gyz", None), P("gx", "gyz", None, None))
    return jax.shard_map(
        on_device, mesh=mesh, in_specs=in_specs, out_specs=out_specs, check_vma=False
    )
```
